32 devices in a mesh: seq: 8 (over y, x, core), exp: 4 (over z).
Axes of the slice: x: 2, y: 2, z: 4, core: 2. Of those that a mesh axis runs over, the one named last changes fastest.
Arguments:
- grad_out: bfloat16 [4096, 2048], P(('seq', 'exp')), may hold values from -6 to 6
- out_proj: bfloat16 [4096, 2048], P('exp'), may hold values from -0.125 to 0.125
- step_size: float32 [64, 4096], P('exp', 'seq'), may hold values from 0.001 to 0.1
- log_decay: float32 [64, 4096], P('exp', 'seq'), may hold values from -1 to 0, as said below
- b_input: float32 [16, 4096], P(None, 'seq'), may hold values from -1.5 to 1.5
- c_output: float32 [16, 4096], P(None, 'seq'), may hold values from -1.5 to 1.5
- skip_gain: float32 [4096], P('exp'), may hold values from 0.5 to 1.5
- expert_ids: int32 [4096, 2], P('seq'), may hold values from 0 to 3, all different within a row; in each aligned block of 128 rows (0 to 127, 128 to 255, ...) at most 66 rows name the same one
- hidden_act: bfloat16 [4, 32, 66, 8192], P('exp', None, None, 'seq'), may hold values from -6 to 6
- w_down: bfloat16 [4, 8192, 2048], P('exp', 'seq'), may hold values from -0.0029296875 to 0.0029296875
Outputs:
- d_inner: bfloat16 [4096, 4096], P('seq', 'exp')
- d_gate: float32 [2, 4096], P(None, ('seq', 'exp'))
The draws below stay inside these ranges and needn't reach their ends.
Inputs may be any that keep to these rules, and one draw needn't show every extreme that they name: `expert_ids`: each row names 2 different experts. Within the rows of one token group no expert is named by more than 66 rows, and in every draw some expert is named by exactly 66 rows of some group. `log_decay`: every entry is negative.
All inputs are finite; a program needn't handle non-finite values.
Results may differ from the reference program's by a relative error of at most 0.00065.
Values may be sent and summed in bfloat16 or wider, within the bound.
A program may use at most 128 MiB of HBM per device.

```python
import math
from functools import partial
import jax
import jax.numpy as jnp
import numpy as np
from jax import lax

D = 2048
INNER = 4096
STATE = 16
HEAD = 64
FF = 8192
TOP = 2
TOK_DEV = 128
EXPERTS = 4
CAP = 66
SEQ_ROWS = 512
SEQUENCE_ITEMS = 4096
SOURCES = 32
HEADS = 64


def draw_log_decay(key, part):
    stochastic_seeds = jax.random.split(key, 7)
    slow_rate = jnp.exp(jax.random.uniform(stochastic_seeds[0], (HEADS, 1), jnp.float32, math.log(0.1 / SEQUENCE_ITEMS), math.log(0.8 / SEQUENCE_ITEMS)))
    fast_rate = jnp.exp(jax.random.uniform(stochastic_seeds[1], (HEADS, 1), jnp.float32, math.log(0.02), math.log(0.05)))
    slow_mask = jax.random.bernoulli(stochastic_seeds[2], 0.5, (HEADS, 1))
    per_channel_forgetting = jnp.where(slow_mask, slow_rate, fast_rate)
    forgetting_noise = jnp.exp(jax.random.uniform(stochastic_seeds[3], (HEADS, SEQUENCE_ITEMS), jnp.float32, math.log(0.5), math.log(2.0)))
    shard_draw = jnp.exp(jax.random.uniform(stochastic_seeds[4], (HEADS, SEQUENCE_ITEMS // SEQ_ROWS), jnp.float32, math.log(0.5), math.log(2.0)))
    shard_multiplier = jnp.repeat(shard_draw, SEQ_ROWS, axis=1)
    spike_opening_slot = jax.random.randint(stochastic_seeds[5], (2, 1), 0, SEQUENCE_ITEMS)
    spike_span = jax.random.uniform(stochastic_seeds[6], (2, 1), jnp.float32, 0.22, 0.45)
    sequence_offsets = lax.broadcasted_iota(jnp.int32, (2, SEQUENCE_ITEMS), 1)
    spike_table = jnp.sum(jnp.where(sequence_offsets == spike_opening_slot, spike_span, 0.0), axis=0)
    return -(per_channel_forgetting * forgetting_noise * shard_multiplier) - spike_table[None, :]


def level_of(rng, dims, shards, low, largest):
    gain = 1.0
    for dim, parts in shards:
        steps = jax.random.uniform(jax.random.fold_in(jax.random.fold_in(rng, 6), dim), (parts,), jnp.float32, low / len(shards), largest / len(shards))
        gain = gain * jnp.repeat(jnp.exp(steps), dims[dim] // parts).reshape((-1,) + (1,) * (len(dims) - 1 - dim))
    return gain


def assign_block(key, own, number, rows, amount, top, limit, skew):
    ranking = jax.random.permutation(key, amount)
    heavy_load, usual = shares(amount, rows * top, limit, skew, True), shares(amount, rows * top, limit, skew, False)
    places = jnp.arange(amount)

    def named(lengths, turn):
        used = int((lengths > 0).sum())
        fixed = max(1, used // 4)
        passed = fixed + (places - fixed + turn * (used - fixed)) % max(1, amount - fixed)
        return jnp.zeros((amount,), jnp.int32).at[ranking[jnp.where(places < fixed, places, passed)]].set(jnp.asarray(lengths, jnp.int32))

    lengths = jnp.where(number % 4 == 0, named(heavy_load, number // 4), named(usual, number - number // 4 - 1))
    mixed = jax.random.permutation(jax.random.fold_in(own, 3), amount)
    giver, taker = mixed[0:amount // 2 * 2:2], mixed[1:amount // 2 * 2:2]
    room = jnp.minimum(lengths[giver] - 1, limit - lengths[taker]) // 2
    room = jnp.where((giver == ranking[0]) | (taker == ranking[0]) | (lengths[taker] == 0), 0, jnp.maximum(room, 0))
    passed = jax.random.randint(jax.random.fold_in(own, 4), (amount // 2,), 0, 1 << 20) % (room + 1)
    lengths = lengths.at[giver].add(-passed).at[taker].add(passed)
    members = jnp.searchsorted(jnp.cumsum(lengths), jnp.arange(rows * top), side="right").astype(jnp.int32)
    table = members.reshape(top, rows).T
    table = table[jax.random.permutation(jax.random.fold_in(own, 1), rows)]
    turn = jax.random.randint(jax.random.fold_in(own, 2), (rows, 1), 0, top)
    return jnp.take_along_axis(table, (jnp.arange(top)[None, :] + turn) % top, axis=1)


def shares(amount, total, limit, slope, full):
    portions = [(1 << 20) // math.isqrt(standing ** slope) + 1 for standing in range(1, amount + 1)]
    largest = limit if full else min(limit, max(-(-total // amount), total * portions[0] // sum(portions)))
    least = 1 if total - largest >= amount - 1 else 0
    given, spare = [largest] + [least] * (amount - 1), total - largest - least * (amount - 1)
    while spare > 0:
        free = [i for i in range(1, amount) if given[i] < largest] or [i for i in range(1, amount) if given[i] < limit]
        mass, remaining = sum([portions[i] for i in free]), spare
        for i in free:
            more = min(limit - given[i], max(1, remaining * portions[i] // mass), spare)
            given[i] = given[i] + more
            spare = spare - more
    return np.array(given)


def normal_values(key, dims, width, bound, cuts=(), kind=jnp.bfloat16):
    entries = width * jax.random.normal(key, dims, jnp.float32)
    if cuts:
        entries = entries * level_of(key, dims, cuts, -0.22, 0.18)
    return jnp.clip(entries, -bound, bound).astype(kind)


def setup_inputs(seed: int = 0) -> dict:
    streams_of = jax.random.split(jax.random.key(seed), 11)
    grad_out = normal_values(streams_of[0], (SEQUENCE_ITEMS, D), 1.0, 6.0, ((0, 32),))
    out_proj = normal_values(streams_of[1], (INNER, D), D ** -0.5, 0.125, ((0, 4),))
    step_size = jnp.clip(jnp.exp(math.log(0.1) - 4.6051702 * jax.random.uniform(streams_of[2], (HEADS, SEQUENCE_ITEMS), jnp.float32) ** level_of(streams_of[2], (HEADS, SEQUENCE_ITEMS), ((0, 4), (1, 8)), -0.2, 0.2)), 0.001, 0.1)
    log_decay = draw_log_decay(jax.random.fold_in(streams_of[10], 71), 0)
    b_input = normal_values(streams_of[4], (STATE, SEQUENCE_ITEMS), 0.25, 1.5, ((1, 8),), jnp.float32)
    c_output = normal_values(streams_of[5], (STATE, SEQUENCE_ITEMS), 0.25, 1.5, ((1, 8),), jnp.float32)
    skip_gain = jnp.clip(0.5 + 1.0 * jax.random.uniform(streams_of[6], (INNER,), jnp.float32) ** level_of(streams_of[6], (INNER,), ((0, 4),), -0.2, 0.2), 0.5, 1.5)
    expert_ids_keys = jax.random.split(jax.random.fold_in(streams_of[7], 1), SEQUENCE_ITEMS // TOK_DEV)
    expert_ids_turns = jax.random.permutation(jax.random.fold_in(streams_of[7], 3), SEQUENCE_ITEMS // TOK_DEV)
    expert_ids = jax.vmap(lambda own, number: assign_block(jax.random.fold_in(streams_of[7], 2), own, number, TOK_DEV, EXPERTS, TOP, CAP, 0))(expert_ids_keys, expert_ids_turns).reshape((SEQUENCE_ITEMS, TOP))
    hidden_act = normal_values(streams_of[8], (EXPERTS, SOURCES, CAP, FF), 1.0, 6.0, ((0, 4), (3, 8)))
    w_down = normal_values(streams_of[9], (EXPERTS, FF, D), (FF * D // 4) ** -0.5, 0.0029296875, ((0, 4), (1, 8)))
    return {"grad_out": grad_out, "out_proj": out_proj, "step_size": step_size, "log_decay": log_decay, "b_input": b_input, "c_output": c_output, "skip_gain": skip_gain, "expert_ids": expert_ids, "hidden_act": hidden_act, "w_down": w_down}


highest = lax.Precision.HIGHEST


def block_pass(state_in, pieces):
    grad_block, decay_block, step_block, b_block, c_block = pieces
    cum_decay = jnp.cumsum(decay_block, axis=1)
    gap_table = cum_decay[:, None, :] - cum_decay[:, :, None]
    upper_mask = lax.broadcasted_iota(jnp.int32, gap_table.shape, 2) >= lax.broadcasted_iota(jnp.int32, gap_table.shape, 1)
    weights = jnp.where(upper_mask, jnp.exp(jnp.where(upper_mask, gap_table, 0.0)), 0.0)
    intersection = lax.dot_general(b_block, c_block, (((0,), (0,)), ((), ())), precision=highest, preferred_element_type=jnp.float32)
    within = jnp.einsum("hut,thp->uhp", weights * intersection[None], grad_block, precision=highest)
    tail_decay = jnp.exp(cum_decay[:, -1:] - cum_decay)
    from_state = jnp.einsum("nu,hnp->uhp", b_block, state_in, precision=highest) * tail_decay.T[:, :, None]
    result = step_block.T[:, :, None] * (within + from_state)
    state_out = jnp.einsum("ht,nt,thp->hnp", jnp.exp(cum_decay), c_block, grad_block, precision=highest)
    state_out = state_out + jnp.exp(cum_decay[:, -1])[:, None, None] * state_in
    return state_out, result


def local_sweep(grad_rows, decay_rows, step_rows, b_rows, c_rows, start_state):
    row_count = grad_rows.shape[0]
    head_count = decay_rows.shape[0]
    block_len = min(512, row_count)
    block_count = row_count // block_len
    pieces = (grad_rows.reshape(block_count, block_len, head_count, grad_rows.shape[2]),
              decay_rows.reshape(head_count, block_count, block_len).transpose(1, 0, 2),
              step_rows.reshape(head_count, block_count, block_len).transpose(1, 0, 2),
              b_rows.reshape(b_rows.shape[0], block_count, block_len).transpose(1, 0, 2),
              c_rows.reshape(c_rows.shape[0], block_count, block_len).transpose(1, 0, 2))
    state_out, results = lax.scan(block_pass, start_state, pieces, reverse=True)
    return state_out, results.reshape(row_count, head_count, grad_rows.shape[2])


def route_table(groups, expert, cap_len):
    hit_mask = jnp.any(groups == expert, axis=2)
    rank_ids = jnp.cumsum(hit_mask.astype(jnp.int32), axis=1) - 1
    slot_ids = lax.broadcasted_iota(jnp.int32, (1, 1, cap_len), 2)
    chosen = jnp.logical_and(hit_mask[:, :, None], rank_ids[:, :, None] == slot_ids)
    token_ids = lax.broadcasted_iota(jnp.int32, chosen.shape, 1)
    position = jnp.sum(jnp.where(chosen, token_ids, 0), axis=1).astype(jnp.int32)
    filled = jnp.any(chosen, axis=1)
    return position, filled


def slot_lookup(slot_table, own_ids, cap_len, expert_count):
    experts_iota = lax.broadcasted_iota(jnp.int32, (1, 1, expert_count), 2)
    onehot = own_ids[:, :, None] == experts_iota
    member = jnp.any(onehot, axis=1).astype(jnp.int32)
    rank_ids = jnp.cumsum(member, axis=0) - 1
    slot_of = jnp.sum(jnp.where(onehot, rank_ids[:, None, :], 0), axis=2)
    picked = jnp.sum(jnp.where(onehot[:, :, :, None], slot_table[None, None], 0.0), axis=2)
    slot_iota = lax.broadcasted_iota(jnp.int32, (1, 1, cap_len), 2)
    return jnp.sum(jnp.where(slot_of[:, :, None] == slot_iota, picked, 0.0), axis=2)


def reference(grad_out, out_proj, step_size, log_decay, b_input, c_output, skip_gain, expert_ids, hidden_act, w_down):
    inner_grad = jnp.dot(grad_out, out_proj.T, preferred_element_type=jnp.float32)
    start_state = jnp.zeros((HEADS, STATE, HEAD), jnp.float32)
    unused, swept_part = local_sweep(inner_grad.reshape(SEQUENCE_ITEMS, HEADS, HEAD), log_decay, step_size, b_input, c_output, start_state)
    d_inner = (swept_part.reshape(SEQUENCE_ITEMS, INNER) + skip_gain * inner_grad).astype(jnp.bfloat16)
    groups = expert_ids.reshape(SOURCES, TOK_DEV, TOP)
    sources = grad_out.reshape(SOURCES, TOK_DEV, D)

    def per_expert(pieces):
        expert, saved_part, weights = pieces
        position, filled = route_table(groups, expert, CAP)
        slot_rows = jnp.take_along_axis(sources, position[:, :, None], axis=1)
        slot_rows = jnp.where(filled[:, :, None], slot_rows, jnp.zeros_like(slot_rows))
        projected = jnp.dot(slot_rows.reshape(SOURCES * CAP, D), weights.T, preferred_element_type=jnp.float32)
        scores = jnp.sum(projected * saved_part.reshape(SOURCES * CAP, FF).astype(jnp.float32), axis=1)
        return scores.reshape(SOURCES, CAP)

    slot_scores = lax.map(per_expert, (jnp.arange(EXPERTS, dtype=jnp.int32), hidden_act, w_down))
    lookup = partial(slot_lookup, cap_len=CAP, expert_count=EXPERTS)
    values = jax.vmap(lookup, in_axes=(1, 0))(slot_scores, groups)
    d_gate = values.reshape(SEQUENCE_ITEMS, TOP).T
    return d_inner, d_gate
```

```python
import functools

import jax
import jax.numpy as jnp
from jax import lax
from jax.experimental import pallas as pl
from jax.experimental.pallas import tpu as pltpu
from jax.sharding import PartitionSpec as P

HEAD = 64


highest = lax.Precision.HIGHEST


def block_pass(state_in, pieces):
    grad_block, decay_block, step_block, b_block, c_block = pieces
    cum_decay = jnp.cumsum(decay_block, axis=1)
    gap_table = cum_decay[:, None, :] - cum_decay[:, :, None]
    upper_mask = lax.broadcasted_iota(jnp.int32, gap_table.shape, 2) >= lax.broadcasted_iota(
        jnp.int32, gap_table.shape, 1
    )
    weights = jnp.where(upper_mask, jnp.exp(jnp.where(upper_mask, gap_table, 0.0)), 0.0)
    intersection = lax.dot_general(
        b_block,
        c_block,
        (((0,), (0,)), ((), ())),
        precision=highest,
        preferred_element_type=jnp.float32,
    )
    within = jnp.einsum("hut,thp->uhp", weights * intersection[None], grad_block, precision=highest)
    tail_decay = jnp.exp(cum_decay[:, -1:] - cum_decay)
    from_state = (
        jnp.einsum("nu,hnp->uhp", b_block, state_in, precision=highest) * tail_decay.T[:, :, None]
    )
    result = step_block.T[:, :, None] * (within + from_state)
    state_out = jnp.einsum(
        "ht,nt,thp->hnp", jnp.exp(cum_decay), c_block, grad_block, precision=highest
    )
    state_out = state_out + jnp.exp(cum_decay[:, -1])[:, None, None] * state_in
    return (state_out, result)


def local_sweep(grad_rows, decay_rows, step_rows, b_rows, c_rows, start_state):
    row_count = grad_rows.shape[0]
    head_count = decay_rows.shape[0]
    block_len = min(512, row_count)
    block_count = row_count // block_len
    pieces = (
        grad_rows.reshape(block_count, block_len, head_count, grad_rows.shape[2]),
        decay_rows.reshape(head_count, block_count, block_len).transpose(1, 0, 2),
        step_rows.reshape(head_count, block_count, block_len).transpose(1, 0, 2),
        b_rows.reshape(b_rows.shape[0], block_count, block_len).transpose(1, 0, 2),
        c_rows.reshape(c_rows.shape[0], block_count, block_len).transpose(1, 0, 2),
    )
    state_out, results = lax.scan(block_pass, start_state, pieces, reverse=True)
    return (state_out, results.reshape(row_count, head_count, grad_rows.shape[2]))


def route_table(groups, expert, cap_len):
    hit_mask = jnp.any(groups == expert, axis=2)
    rank_ids = jnp.cumsum(hit_mask.astype(jnp.int32), axis=1) - 1
    slot_ids = lax.broadcasted_iota(jnp.int32, (1, 1, cap_len), 2)
    chosen = jnp.logical_and(hit_mask[:, :, None], rank_ids[:, :, None] == slot_ids)
    token_ids = lax.broadcasted_iota(jnp.int32, chosen.shape, 1)
    position = jnp.sum(jnp.where(chosen, token_ids, 0), axis=1)
    filled = jnp.any(chosen, axis=1)
    return (position, filled)


def slot_lookup(slot_table, own_ids, cap_len, expert_count):
    experts_iota = lax.broadcasted_iota(jnp.int32, (1, 1, expert_count), 2)
    onehot = own_ids[:, :, None] == experts_iota
    member = jnp.any(onehot, axis=1).astype(jnp.int32)
    rank_ids = jnp.cumsum(member, axis=0) - 1
    slot_of = jnp.sum(jnp.where(onehot, rank_ids[:, None, :], 0), axis=2)
    picked = jnp.sum(jnp.where(onehot[:, :, :, None], slot_table[None, None], 0.0), axis=2)
    slot_iota = lax.broadcasted_iota(jnp.int32, (1, 1, cap_len), 2)
    return jnp.sum(jnp.where(slot_of[:, :, None] == slot_iota, picked, 0.0), axis=2)


def shards(
    grad_out,
    out_proj,
    step_size,
    log_decay,
    b_input,
    c_output,
    skip_gain,
    expert_ids,
    hidden_act,
    w_down,
):
    exp_index = lax.axis_index("exp")
    seq_index = lax.axis_index("seq")
    exp_count = lax.axis_size("exp")
    seq_count = lax.axis_size("seq")
    tok_len = grad_out.shape[0]
    cap_len = hidden_act.shape[2]
    gathered = lax.all_gather(grad_out, "exp", axis=0, tiled=True)
    groups = expert_ids.reshape(exp_count, tok_len, expert_ids.shape[1])
    position, filled = route_table(groups, exp_index, cap_len)
    flat_index = (position + lax.broadcasted_iota(jnp.int32, position.shape, 0) * tok_len).reshape(
        -1
    )
    slot_rows = jnp.take(gathered, flat_index, axis=0)
    slot_rows = jnp.where(filled.reshape(-1, 1), slot_rows, jnp.zeros_like(slot_rows))
    saved_rows = hidden_act.reshape(-1, hidden_act.shape[3])
    weights = w_down[0]
    projected = lax.dot_general(
        lax.all_gather(slot_rows, "seq", axis=0, tiled=True),
        weights,
        (((1,), (1,)), ((), ())),
        preferred_element_type=jnp.float32,
    )
    partial_scores = jnp.sum(projected * saved_rows.astype(jnp.float32), axis=1)
    head_count = out_proj.shape[0] // HEAD
    inner_grad = lax.dot_general(
        gathered, out_proj, (((1,), (1,)), ((), ())), preferred_element_type=jnp.float32
    )
    row_count = inner_grad.shape[0]
    start_state = jnp.zeros((head_count, b_input.shape[0], HEAD), jnp.float32)
    summary, swept_part = local_sweep(
        inner_grad.reshape(row_count, head_count, HEAD),
        log_decay,
        step_size,
        b_input,
        c_output,
        start_state,
    )
    total_decay = jnp.sum(log_decay, axis=1)
    all_states, all_decay = (
        lax.all_gather(summary[None], "seq", axis=0, tiled=True),
        lax.all_gather(total_decay[None], "seq", axis=0, tiled=True),
    )
    shard_ids = lax.broadcasted_iota(jnp.int32, all_decay.shape, 0)
    beyond = jnp.where(shard_ids > seq_index, all_decay, 0.0)
    exponent = jnp.cumsum(beyond, axis=0) - beyond
    factor = jnp.where(
        shard_ids > seq_index, jnp.exp(jnp.where(shard_ids > seq_index, exponent, 0.0)), 0.0
    )
    incoming = jnp.sum(factor[:, :, None, None] * all_states, axis=0)
    suffix = jnp.flip(jnp.cumsum(jnp.flip(log_decay, 1), axis=1), 1) - log_decay
    from_carry = (
        jnp.einsum("nu,hnp->uhp", b_input, incoming, precision=highest)
        * jnp.exp(suffix).T[:, :, None]
    )
    combined = swept_part + step_size.T[:, :, None] * from_carry
    d_inner = (combined.reshape(row_count, -1) + skip_gain * inner_grad).astype(jnp.bfloat16)
    summed = lax.psum_scatter(
        partial_scores.reshape(seq_count, exp_count, cap_len),
        "seq",
        scatter_dimension=0,
        tiled=True,
    )
    slot_table = lax.all_to_all(
        summed.reshape(exp_count, 1, cap_len), "exp", split_axis=0, concat_axis=1, tiled=True
    ).reshape(exp_count, cap_len)
    own_ids = lax.dynamic_slice_in_dim(expert_ids, exp_index * tok_len, tok_len, 0)
    d_gate = slot_lookup(slot_table, own_ids, cap_len, exp_count).T
    return (d_inner, d_gate)


VMEM_ROOM = 60 << 20
BF = jnp.bfloat16
F32 = jnp.float32


def halves(x):
    top = x.astype(BF)
    return top, (x - top.astype(F32)).astype(BF)


def dot(x, y, dims=((1,), (0,)), precision=None):
    return lax.dot_general(x, y, (dims, ((), ())), precision=precision, preferred_element_type=F32)


def flip(index, bit):
    return index + bit - 2 * bit * ((index // bit) % 2)


def column(table, h):
    lanes = lax.broadcasted_iota(jnp.int32, table.shape, 1)
    return jnp.sum(jnp.where(lanes == h, table, 0.0), axis=1, keepdims=True)


def fused(
    sizes,
    grad_hbm, proj_hbm, hid_hbm, down_hbm, step_ref, decay_ref, b_ref, c_ref, skip_ref, ids_ref,
    out_ref, score_ref,
    gath, proj, hid, down, y_ref, rows, hid_pad, pick, inner, fac, acc,
    cum_ref, cum_t, step_t, b_t, bc, agg, got, carry,
    load_sem, hid_sem, down_sem, proj_sem,
    zs_sem, zr_sem, xs_sem, xr_sem, as_sem, ar_sem,
):
    n_seq, n_exp, tok, cap, pad, chunks, width = sizes
    me = lax.axis_index("seq")
    z = lax.axis_index("exp")
    shard = n_exp * pad
    row_count = n_exp * tok
    bits = [1 << i for i in range(1, n_seq.bit_length() - 1)]
    n_stage = len(bits)
    steps = n_exp - 1
    block = bc.shape[1]
    blocks = row_count // block
    channels = inner.shape[1]
    lane = 2 * HEAD
    pairs = channels // lane

    for k in range(chunks):
        pltpu.make_async_copy(
            grad_hbm.at[:, pl.ds(k * width, width)], gath.at[k, z], load_sem.at[k]
        ).start()
    down_copy = pltpu.make_async_copy(down_hbm.at[0], down, down_sem)
    down_copy.start()
    hid_copy = pltpu.make_async_copy(hid_hbm.at[0], hid, hid_sem)
    hid_copy.start()
    for k in range(chunks):
        pltpu.make_async_copy(
            proj_hbm.at[:, pl.ds(k * width, width)], proj.at[k], proj_sem.at[k]
        ).start()

    barrier = pltpu.get_barrier_semaphore()
    for bit in [1] + bits:
        pl.semaphore_signal(barrier, inc=1, device_id={"seq": flip(me, bit)})

    @pl.when(z > 0)
    def _():
        pl.semaphore_signal(barrier, inc=1, device_id={"exp": z - 1})

    @pl.when(z < n_exp - 1)
    def _():
        pl.semaphore_signal(barrier, inc=1, device_id={"exp": z + 1})

    ends = jnp.minimum(z, 1) + jnp.minimum(n_exp - 1 - z, 1)
    pl.semaphore_wait(barrier, n_stage + 1 + ends)

    def z_copy(side, k, d, owner, target):
        return pltpu.make_async_remote_copy(
            src_ref=gath.at[k, owner],
            dst_ref=gath.at[k, owner],
            send_sem=zs_sem.at[side, k, d],
            recv_sem=zr_sem.at[side, k, d],
            device_id={"exp": target},
        )

    def z_send(k, d):
        @pl.when(jnp.logical_and(z < n_exp - 1, z - d >= 0))
        def _():
            z_copy(0, k, d, z - d, z + 1).start()

        @pl.when(jnp.logical_and(z > 0, z + d < n_exp))
        def _():
            z_copy(1, k, d, z + d, z - 1).start()

    def z_sent(k, d):
        @pl.when(jnp.logical_and(z < n_exp - 1, z - d >= 0))
        def _():
            z_copy(0, k, d, z - d, z + 1).wait_send()

        @pl.when(jnp.logical_and(z > 0, z + d < n_exp))
        def _():
            z_copy(1, k, d, z + d, z - 1).wait_send()

    def z_take(k, d):
        @pl.when(z - d >= 0)
        def _():
            z_copy(0, k, d - 1, z - d, z).wait_recv()

        @pl.when(z + d < n_exp)
        def _():
            z_copy(1, k, d - 1, z + d, z).wait_recv()

    for k in range(chunks):
        pltpu.make_async_copy(
            grad_hbm.at[:, pl.ds(k * width, width)], gath.at[k, z], load_sem.at[k]
        ).wait()
        z_send(k, 0)

    def bit_of(k, stage):
        if stage == n_stage:
            return 1
        low, high = bits[stage], bits[n_stage - 1 - stage]
        return low + (high - low) * (k % 2)

    def x_copies(k, stage, here):
        masks = [()]
        for i in range(stage):
            masks = masks + [m + (i,) for m in masks]
        copies = []
        for j, mask in enumerate(masks):
            owner = me
            for i in mask:
                owner = flip(owner, bit_of(k, i))
            slot = (1 << stage) - 1 + j
            if not here:
                owner = flip(owner, bit_of(k, stage))
            copies.append(pltpu.make_async_remote_copy(
                src_ref=rows.at[k, owner],
                dst_ref=rows.at[k, owner],
                send_sem=xs_sem.at[k, slot],
                recv_sem=xr_sem.at[k, slot],
                device_id={"seq": flip(me, bit_of(k, stage))},
            ))
        return copies

    def x_start(k, stage):
        for mine in x_copies(k, stage, True):
            mine.start()

    def x_take(k, stage):
        for theirs in x_copies(k, stage, False):
            theirs.wait_recv()

    ids = ids_ref[...]
    hit = jnp.where(jnp.logical_or(ids[:, 0:1] == z, ids[:, 1:2] == z), 1.0, 0.0)
    for i in range(2, ids.shape[1]):
        hit = jnp.maximum(hit, jnp.where(ids[:, i : i + 1] == z, 1.0, 0.0))
    row_id = lax.broadcasted_iota(jnp.int32, (row_count, row_count), 0)
    col_id = lax.broadcasted_iota(jnp.int32, (row_count, row_count), 1)
    same = jnp.logical_and(row_id // tok == col_id // tok, col_id < row_id)
    before = dot(jnp.where(same, 1.0, 0.0).astype(BF), jnp.broadcast_to(hit, (row_count, 128)).astype(BF))
    group = lax.broadcasted_iota(jnp.int32, (row_count, 1), 0) // tok
    place = before[:, 0:1].astype(jnp.int32) + group * pad
    slots = -(-shard // 128) * 128
    chosen = jnp.logical_and(
        lax.broadcasted_iota(jnp.int32, (row_count, slots), 1) == place, hit > 0.5
    )
    pick[...] = jnp.transpose(jnp.where(chosen, 1.0, 0.0))[:shard].astype(BF)

    tri = jnp.where(row_id <= col_id, 1.0, 0.0)
    cum = dot(decay_ref[...], tri, precision=highest)
    cum_ref[...] = cum
    cum_t[...] = jnp.transpose(cum)
    step_t[...] = jnp.transpose(step_ref[...])
    b_t[...] = jnp.transpose(b_ref[...])
    keep = lax.broadcasted_iota(jnp.int32, (block, block), 1) >= lax.broadcasted_iota(
        jnp.int32, (block, block), 0
    )
    for i in range(blocks):
        span = slice(i * block, (i + 1) * block)
        cross = dot(b_t[span, :], c_ref[:, span], precision=highest)
        bc[i] = jnp.where(keep, cross, 0.0)

    hid_pad[...] = jnp.zeros_like(hid_pad)
    inner[...] = jnp.zeros_like(inner)
    acc[...] = jnp.zeros_like(acc)
    down_copy.wait()
    hid_copy.wait()

    def project(s):
        for g in range(n_exp):
            hid_pad[g * pad : g * pad + cap, :] = hid[s * n_exp + g].astype(F32)
        saved = hid_pad[...].astype(BF)
        for k in range(chunks):
            y_ref[k, s] = dot(saved, down[:, k * width : (k + 1) * width])

    def z_step(i, _):
        k, d = i // steps, i % steps + 1

        @pl.when(i < n_seq)
        def _():
            project(i)

        z_take(k, d)

        @pl.when(d < steps)
        def _():
            z_send(k, d)

        @pl.when(d == steps)
        def _():
            block_in = gath[k].reshape(row_count, width)
            rows[k, me] = dot(pick[...], block_in).astype(BF)
            x_start(k, 0)

            @pl.when(k >= 1)
            def _():
                x_take(k - 1, 0)
                x_start(k - 1, 1)

            pltpu.make_async_copy(
                proj_hbm.at[:, pl.ds(0, width)], proj.at[k], proj_sem.at[k]
            ).wait()
            inner[...] += dot(gath[k].reshape(row_count, width), proj[k], ((1,), (1,)))

        return 0

    lax.fori_loop(0, chunks * steps, z_step, 0)
    for s in range(chunks * steps, n_seq):
        project(s)

    left_of = lax.broadcasted_iota(jnp.int32, (1, lane), 1) < HEAD

    def pair_step(j, _):
        span = pl.ds(pl.multiple_of(j * lane, lane), lane)
        cols = [column(cum_t[...], 2 * j + i) for i in range(2)]
        rowv = [cum_ref[pl.ds(2 * j + i, 1), :] for i in range(2)]
        steps_col = jnp.where(
            left_of, column(step_t[...], 2 * j), column(step_t[...], 2 * j + 1)
        )
        col = jnp.where(left_of, cols[0], cols[1])
        end_row = jnp.where(left_of, cols[0][row_count - 1 :], cols[1][row_count - 1 :])
        fac[:, span] = steps_col * jnp.exp(end_row - col)
        skip = skip_ref[:, span]
        state = jnp.zeros((b_t.shape[1], lane), F32)
        for i in reversed(range(blocks)):
            lo, hi = i * block, (i + 1) * block
            g = inner[lo:hi, span]
            g_top, g_low = halves(g)
            both = jnp.concatenate([g_top, g_low], axis=1)
            parts, sums = [], []
            for q in range(2):
                r = rowv[q][:, lo:hi]
                w = jnp.exp(jnp.minimum(r - cols[q][lo:hi], 0.0)) * bc[i]
                w_top, w_low = halves(w)
                x = dot(w_top, both)
                parts.append(x[:, :lane] + x[:, lane:] + dot(w_low, g_top))
                base = rowv[q][:, lo - 1 : lo] if i else jnp.zeros((1, 1), F32)
                m_top, m_low = halves(c_ref[:, lo:hi] * jnp.exp(r - base))
                x = dot(m_top, both)
                sums.append(x[:, :lane] + x[:, lane:] + dot(m_low, g_top))
            result = jnp.where(left_of, parts[0], parts[1])
            if i < blocks - 1:
                edge = col[hi - 1 : hi]
                result += jnp.exp(edge - col[lo:hi]) * dot(b_t[lo:hi, :], state, precision=highest)
            start = col[lo - 1 : lo] if i else jnp.zeros((1, lane), F32)
            state = jnp.where(left_of, sums[0], sums[1]) + jnp.exp(col[hi - 1 : hi] - start) * state
            inner[lo:hi, span] = steps_col[lo:hi] * result + skip * g
        agg[0, : b_t.shape[1], span] = state
        agg[0, b_t.shape[1] :, span] = jnp.broadcast_to(end_row, (8, lane))
        return 0

    def scores(k):
        def one(s, _):
            part = rows[k, s].astype(F32) * y_ref[k, s]
            total = part[:, :128]
            for i in range(1, width // 128):
                total = total + part[:, i * 128 : (i + 1) * 128]
            acc[s] += total
            return 0

        lax.fori_loop(0, n_seq, one, 0)

    tasks = []
    for stage in range(1, n_stage + 1):
        for k in range(chunks):
            if stage > 1 or k == chunks - 1:
                tasks.append((k, stage))
    tasks.sort(key=lambda t: (t[0] + 1.5 * t[1], t[0]))

    def serve(count):
        for _ in range(min(count, len(tasks))):
            k, stage = tasks.pop(0)
            x_take(k, stage - 1)
            x_start(k, stage)

    serve(1)
    cut = pairs // 2
    lax.fori_loop(0, cut, pair_step, 0)
    serve(1)
    lax.fori_loop(cut, pairs, pair_step, 0)

    n_state = b_t.shape[1]
    carry[...] = jnp.zeros_like(carry)
    reach = jnp.zeros((1, channels), F32)

    def a_copy(i, bit):
        return pltpu.make_async_remote_copy(
            src_ref=agg.at[i],
            dst_ref=got.at[i],
            send_sem=as_sem.at[i],
            recv_sem=ar_sem.at[i],
            device_id={"seq": flip(me, bit)},
        )

    order = [1] + bits
    a_copy(0, 1).start()
    for i, bit in enumerate(order):
        serve(1)
        a_copy(i, bit).wait_recv()
        low = ((me // bit) % 2) == 0
        other, other_t = got[i, :n_state, :], got[i, n_state : n_state + 1, :]
        own, own_t = agg[i, :n_state, :], agg[i, n_state : n_state + 1, :]
        carry[...] += jnp.where(low, jnp.exp(reach) * other, 0.0)
        reach = reach + jnp.where(low, other_t, 0.0)
        if i + 1 < len(order):
            first = jnp.where(low, own, other)
            first_t = jnp.where(low, own_t, other_t)
            second = jnp.where(low, other, own)
            agg[i + 1, :n_state, :] = first + jnp.exp(first_t) * second
            agg[i + 1, n_state:, :] = jnp.broadcast_to(own_t + other_t, (8, channels))
            a_copy(i + 1, order[i + 1]).start()

    for i in range(blocks):
        lo, hi = i * block, (i + 1) * block
        from_carry = dot(b_t[lo:hi, :], carry[...], precision=highest)
        out_ref[lo:hi, :] = (inner[lo:hi, :] + fac[lo:hi, :] * from_carry).astype(BF)

    ready = [k for k in range(chunks) if (k, n_stage) not in tasks]
    for k in range(chunks):
        if k not in ready:
            while (k, n_stage) in tasks:
                serve(1)
        x_take(k, n_stage)
        scores(k)

    def finish(s, _):
        wide = jnp.transpose(acc[s])
        score_ref[s] = jnp.sum(wide, axis=0, keepdims=True)
        return 0

    lax.fori_loop(0, n_seq, finish, 0)

    for k in range(chunks):
        for d in range(steps):
            z_sent(k, d)
        for stage in range(n_stage + 1):
            for mine in x_copies(k, stage, True):
                mine.wait_send()
    for i, bit in enumerate(order):
        a_copy(i, bit).wait_send()


def plan(n_seq, n_exp, tok, depth, channels, cap, hidden, state):
    pad = -(-cap // 8) * 8
    chunks = 4
    width = depth // chunks
    shard = n_exp * pad
    row_count = n_exp * tok
    block = min(256, row_count)
    heads = channels // HEAD
    stages = n_seq.bit_length() - 1
    steps = n_exp - 1
    shapes = [
        ((chunks, n_exp, tok, width), BF),
        ((chunks, channels, width), BF),
        ((n_seq * n_exp, cap, hidden), BF),
        ((hidden, depth), BF),
        ((chunks, n_seq, shard, width), F32),
        ((chunks, n_seq, shard, width), BF),
        ((shard, hidden), F32),
        ((shard, row_count), BF),
        ((row_count, channels), F32),
        ((row_count, channels), F32),
        ((n_seq, shard, 128), F32),
        ((heads, row_count), F32),
        ((row_count, heads), F32),
        ((row_count, heads), F32),
        ((row_count, state), F32),
        ((row_count // block, block, block), F32),
        ((stages, state + 8, channels), F32),
        ((stages, state + 8, channels), F32),
        ((state, channels), F32),
    ]
    total = 0
    for shape, kind in shapes:
        size = 1
        for extent in shape:
            size *= extent
        total += size * (2 if kind is BF else 4)
    fits = (
        total < VMEM_ROOM - (8 << 20)
        and n_seq & (n_seq - 1) == 0
        and n_seq >= 4
        and n_exp >= 2
        and depth % (128 * chunks) == 0
        and channels % (2 * HEAD) == 0
        and row_count % block == 0
        and tok % 8 == 0
    )
    sems = [
        (chunks,), (), (), (chunks,),
        (2, chunks, steps), (2, chunks, steps),
        (chunks, n_seq - 1), (chunks, n_seq - 1),
        (stages,), (stages,),
    ]
    return fits, (n_seq, n_exp, tok, cap, pad, chunks, width), shapes, sems


def quick(
    fitted, grad_out, out_proj, step_size, log_decay, b_input, c_output, skip_gain, expert_ids,
    hidden_act, w_down,
):
    _, sizes, shapes, sems = fitted
    n_seq, n_exp, tok, cap, pad, chunks, width = sizes
    shard = n_exp * pad
    vmem = pl.BlockSpec(memory_space=pltpu.VMEM)
    hbm = pl.BlockSpec(memory_space=pl.ANY)
    row_count, channels = n_exp * tok, out_proj.shape[0]
    d_inner, table = pl.pallas_call(
        functools.partial(fused, sizes),
        out_shape=(
            jax.ShapeDtypeStruct((row_count, channels), BF),
            jax.ShapeDtypeStruct((n_seq, 1, shard), F32),
        ),
        in_specs=[hbm] * 4 + [vmem] * 6,
        out_specs=(vmem, vmem),
        scratch_shapes=[pltpu.VMEM(shape, kind) for shape, kind in shapes]
        + [pltpu.SemaphoreType.DMA(s) if s else pltpu.SemaphoreType.DMA for s in sems],
        compiler_params=pltpu.CompilerParams(
            collective_id=0, has_side_effects=True, vmem_limit_bytes=VMEM_ROOM
        ),
    )(
        grad_out, out_proj, hidden_act, w_down, step_size, log_decay, b_input, c_output,
        skip_gain.reshape(1, -1), expert_ids,
    )
    exchanged = lax.all_to_all(
        table.reshape(n_seq * n_exp, pad), ("seq", "exp"), split_axis=0, concat_axis=0, tiled=True
    )
    slot_table = jnp.sum(exchanged.reshape(n_seq, n_exp, pad), axis=0)
    own_ids = lax.dynamic_slice_in_dim(expert_ids, lax.axis_index("exp") * tok, tok, 0)
    d_gate = slot_lookup(slot_table, own_ids, pad, n_exp).T
    return d_inner, d_gate


def route(*args):
    grad_out, out_proj, step_size, log_decay, b_input, c_output, skip_gain, ids, hidden, down = args
    fitted = plan(
        lax.axis_size("seq"), lax.axis_size("exp"), grad_out.shape[0], grad_out.shape[1],
        out_proj.shape[0], hidden.shape[2], hidden.shape[3], b_input.shape[0],
    )
    if fitted[0]:
        return quick(fitted, *args)
    return shards(*args)


def solution(mesh):
    in_specs = (
        P(("seq", "exp"), None),
        P("exp", None),
        P("exp", "seq"),
        P("exp", "seq"),
        P(None, "seq"),
        P(None, "seq"),
        P("exp"),
        P("seq", None),
        P("exp", None, None, "seq"),
        P("exp", "seq", None),
    )
    out_specs = (P("seq", "exp"), P(None, ("seq", "exp")))
    return jax.shard_map(route, mesh=mesh, in_specs=in_specs, out_specs=out_specs, check_vma=False)
```

```python
import functools

import jax
import jax.numpy as jnp
from jax import lax
from jax.experimental import pallas as pl
from jax.experimental.pallas import tpu as pltpu
from jax.sharding import PartitionSpec as P

HEAD = 64


highest = lax.Precision.HIGHEST


def block_pass(state_in, pieces):
    grad_block, decay_block, step_block, b_block, c_block = pieces
    cum_decay = jnp.cumsum(decay_block, axis=1)
    gap_table = cum_decay[:, None, :] - cum_decay[:, :, None]
    upper_mask = lax.broadcasted_iota(jnp.int32, gap_table.shape, 2) >= lax.broadcasted_iota(
        jnp.int32, gap_table.shape, 1
    )
    weights = jnp.where(upper_mask, jnp.exp(jnp.where(upper_mask, gap_table, 0.0)), 0.0)
    intersection = lax.dot_general(
        b_block,
        c_block,
        (((0,), (0,)), ((), ())),
        precision=highest,
        preferred_element_type=jnp.float32,
    )
    within = jnp.einsum("hut,thp->uhp", weights * intersection[None], grad_block, precision=highest)
    tail_decay = jnp.exp(cum_decay[:, -1:] - cum_decay)
    from_state = (
        jnp.einsum("nu,hnp->uhp", b_block, state_in, precision=highest) * tail_decay.T[:, :, None]
    )
    result = step_block.T[:, :, None] * (within + from_state)
    state_out = jnp.einsum(
        "ht,nt,thp->hnp", jnp.exp(cum_decay), c_block, grad_block, precision=highest
    )
    state_out = state_out + jnp.exp(cum_decay[:, -1])[:, None, None] * state_in
    return (state_out, result)


def local_sweep(grad_rows, decay_rows, step_rows, b_rows, c_rows, start_state):
    row_count = grad_rows.shape[0]
    head_count = decay_rows.shape[0]
    block_len = min(512, row_count)
    block_count = row_count // block_len
    pieces = (
        grad_rows.reshape(block_count, block_len, head_count, grad_rows.shape[2]),
        decay_rows.reshape(head_count, block_count, block_len).transpose(1, 0, 2),
        step_rows.reshape(head_count, block_count, block_len).transpose(1, 0, 2),
        b_rows.reshape(b_rows.shape[0], block_count, block_len).transpose(1, 0, 2),
        c_rows.reshape(c_rows.shape[0], block_count, block_len).transpose(1, 0, 2),
    )
    state_out, results = lax.scan(block_pass, start_state, pieces, reverse=True)
    return (state_out, results.reshape(row_count, head_count, grad_rows.shape[2]))


def route_table(groups, expert, cap_len):
    hit_mask = jnp.any(groups == expert, axis=2)
    rank_ids = jnp.cumsum(hit_mask.astype(jnp.int32), axis=1) - 1
    slot_ids = lax.broadcasted_iota(jnp.int32, (1, 1, cap_len), 2)
    chosen = jnp.logical_and(hit_mask[:, :, None], rank_ids[:, :, None] == slot_ids)
    token_ids = lax.broadcasted_iota(jnp.int32, chosen.shape, 1)
    position = jnp.sum(jnp.where(chosen, token_ids, 0), axis=1)
    filled = jnp.any(chosen, axis=1)
    return (position, filled)


def slot_lookup(slot_table, own_ids, cap_len, expert_count):
    experts_iota = lax.broadcasted_iota(jnp.int32, (1, 1, expert_count), 2)
    onehot = own_ids[:, :, None] == experts_iota
    member = jnp.any(onehot, axis=1).astype(jnp.int32)
    rank_ids = jnp.cumsum(member, axis=0) - 1
    slot_of = jnp.sum(jnp.where(onehot, rank_ids[:, None, :], 0), axis=2)
    picked = jnp.sum(jnp.where(onehot[:, :, :, None], slot_table[None, None], 0.0), axis=2)
    slot_iota = lax.broadcasted_iota(jnp.int32, (1, 1, cap_len), 2)
    return jnp.sum(jnp.where(slot_of[:, :, None] == slot_iota, picked, 0.0), axis=2)


def shards(
    grad_out,
    out_proj,
    step_size,
    log_decay,
    b_input,
    c_output,
    skip_gain,
    expert_ids,
    hidden_act,
    w_down,
):
    exp_index = lax.axis_index("exp")
    seq_index = lax.axis_index("seq")
    exp_count = lax.axis_size("exp")
    seq_count = lax.axis_size("seq")
    tok_len = grad_out.shape[0]
    cap_len = hidden_act.shape[2]
    gathered = lax.all_gather(grad_out, "exp", axis=0, tiled=True)
    groups = expert_ids.reshape(exp_count, tok_len, expert_ids.shape[1])
    position, filled = route_table(groups, exp_index, cap_len)
    flat_index = (position + lax.broadcasted_iota(jnp.int32, position.shape, 0) * tok_len).reshape(
        -1
    )
    slot_rows = jnp.take(gathered, flat_index, axis=0)
    slot_rows = jnp.where(filled.reshape(-1, 1), slot_rows, jnp.zeros_like(slot_rows))
    saved_rows = hidden_act.reshape(-1, hidden_act.shape[3])
    weights = w_down[0]
    projected = lax.dot_general(
        lax.all_gather(slot_rows, "seq", axis=0, tiled=True),
        weights,
        (((1,), (1,)), ((), ())),
        preferred_element_type=jnp.float32,
    )
    partial_scores = jnp.sum(projected * saved_rows.astype(jnp.float32), axis=1)
    head_count = out_proj.shape[0] // HEAD
    inner_grad = lax.dot_general(
        gathered, out_proj, (((1,), (1,)), ((), ())), preferred_element_type=jnp.float32
    )
    row_count = inner_grad.shape[0]
    start_state = jnp.zeros((head_count, b_input.shape[0], HEAD), jnp.float32)
    summary, swept_part = local_sweep(
        inner_grad.reshape(row_count, head_count, HEAD),
        log_decay,
        step_size,
        b_input,
        c_output,
        start_state,
    )
    total_decay = jnp.sum(log_decay, axis=1)
    all_states, all_decay = (
        lax.all_gather(summary[None], "seq", axis=0, tiled=True),
        lax.all_gather(total_decay[None], "seq", axis=0, tiled=True),
    )
    shard_ids = lax.broadcasted_iota(jnp.int32, all_decay.shape, 0)
    beyond = jnp.where(shard_ids > seq_index, all_decay, 0.0)
    exponent = jnp.cumsum(beyond, axis=0) - beyond
    factor = jnp.where(
        shard_ids > seq_index, jnp.exp(jnp.where(shard_ids > seq_index, exponent, 0.0)), 0.0
    )
    incoming = jnp.sum(factor[:, :, None, None] * all_states, axis=0)
    suffix = jnp.flip(jnp.cumsum(jnp.flip(log_decay, 1), axis=1), 1) - log_decay
    from_carry = (
        jnp.einsum("nu,hnp->uhp", b_input, incoming, precision=highest)
        * jnp.exp(suffix).T[:, :, None]
    )
    combined = swept_part + step_size.T[:, :, None] * from_carry
    d_inner = (combined.reshape(row_count, -1) + skip_gain * inner_grad).astype(jnp.bfloat16)
    summed = lax.psum_scatter(
        partial_scores.reshape(seq_count, exp_count, cap_len),
        "seq",
        scatter_dimension=0,
        tiled=True,
    )
    slot_table = lax.all_to_all(
        summed.reshape(exp_count, 1, cap_len), "exp", split_axis=0, concat_axis=1, tiled=True
    ).reshape(exp_count, cap_len)
    own_ids = lax.dynamic_slice_in_dim(expert_ids, exp_index * tok_len, tok_len, 0)
    d_gate = slot_lookup(slot_table, own_ids, cap_len, exp_count).T
    return (d_inner, d_gate)


VMEM_ROOM = 60 << 20
BF = jnp.bfloat16
F32 = jnp.float32


def halves(x):
    top = x.astype(BF)
    return top, (x - top.astype(F32)).astype(BF)


def dot(x, y, dims=((1,), (0,)), precision=None):
    return lax.dot_general(x, y, (dims, ((), ())), precision=precision, preferred_element_type=F32)


def flip(index, bit):
    return index + bit - 2 * bit * ((index // bit) % 2)


def column(table, h):
    lanes = lax.broadcasted_iota(jnp.int32, table.shape, 1)
    return jnp.sum(jnp.where(lanes == h, table, 0.0), axis=1, keepdims=True)


def fused(
    sizes,
    grad_hbm, proj_hbm, hid_hbm, down_hbm, step_ref, decay_ref, b_ref, c_ref, skip_ref, ids_ref,
    out_ref, table_ref,
    gath, proj, hid, down, y_ref, rows, pick, inner, fac, acc,
    cum_ref, cum_t, step_t, b_t, bc, agg, got, carry, mail, inbox,
    load_sem, hid_sem, down_sem, proj_sem,
    zs_sem, zr_sem, xs_sem, xr_sem, as_sem, ar_sem, ms_sem, mr_sem,
):
    n_seq, n_exp, tok, cap, shard, chunks, width = sizes
    me = lax.axis_index("seq")
    z = lax.axis_index("exp")
    row_count = n_exp * tok
    spread = 2 * n_exp
    n_dev = n_seq * n_exp
    mine_id = me * n_exp + z
    bits = [1 << i for i in range(1, n_seq.bit_length() - 1)]
    n_stage = len(bits)
    steps = n_exp - 1
    block = bc.shape[1]
    blocks = row_count // block
    channels = inner.shape[1]
    lane = 2 * HEAD
    pairs = channels // lane

    for k in range(chunks):
        pltpu.make_async_copy(
            grad_hbm.at[:, pl.ds(k * width, width)], gath.at[k, z], load_sem.at[k]
        ).start()
    down_copy = pltpu.make_async_copy(down_hbm.at[0], down, down_sem)
    down_copy.start()
    hid_copy = pltpu.make_async_copy(hid_hbm.at[0], hid, hid_sem)
    hid_copy.start()
    for k in range(chunks):
        pltpu.make_async_copy(
            proj_hbm.at[:, pl.ds(k * width, width)], proj.at[k], proj_sem.at[k]
        ).start()

    barrier = pltpu.get_barrier_semaphore()

    def greet(i, _):
        other = lax.rem(mine_id + i, n_dev)
        pl.semaphore_signal(
            barrier, inc=1, device_id={"seq": other // n_exp, "exp": lax.rem(other, n_exp)}
        )
        return 0

    lax.fori_loop(1, n_dev, greet, 0)
    pl.semaphore_wait(barrier, n_dev - 1)

    def z_copy(side, k, d, owner, target):
        return pltpu.make_async_remote_copy(
            src_ref=gath.at[k, owner],
            dst_ref=gath.at[k, owner],
            send_sem=zs_sem.at[side, k, d],
            recv_sem=zr_sem.at[side, k, d],
            device_id={"exp": target},
        )

    def z_send(k, d):
        @pl.when(jnp.logical_and(z < n_exp - 1, z - d >= 0))
        def _():
            z_copy(0, k, d, z - d, z + 1).start()

        @pl.when(jnp.logical_and(z > 0, z + d < n_exp))
        def _():
            z_copy(1, k, d, z + d, z - 1).start()

    def z_sent(k, d):
        @pl.when(jnp.logical_and(z < n_exp - 1, z - d >= 0))
        def _():
            z_copy(0, k, d, z - d, z + 1).wait_send()

        @pl.when(jnp.logical_and(z > 0, z + d < n_exp))
        def _():
            z_copy(1, k, d, z + d, z - 1).wait_send()

    def z_take(k, d):
        @pl.when(z - d >= 0)
        def _():
            z_copy(0, k, d - 1, z - d, z).wait_recv()

        @pl.when(z + d < n_exp)
        def _():
            z_copy(1, k, d - 1, z + d, z).wait_recv()

    for k in range(chunks):
        pltpu.make_async_copy(
            grad_hbm.at[:, pl.ds(k * width, width)], gath.at[k, z], load_sem.at[k]
        ).wait()
        z_send(k, 0)

    def bit_of(k, stage):
        if stage == n_stage:
            return 1
        low, high = bits[stage], bits[n_stage - 1 - stage]
        return low + (high - low) * (k % 2)

    def x_copies(k, stage, here):
        masks = [()]
        for i in range(stage):
            masks = masks + [m + (i,) for m in masks]
        copies = []
        for j, mask in enumerate(masks):
            owner = me
            for i in mask:
                owner = flip(owner, bit_of(k, i))
            slot = (1 << stage) - 1 + j
            if not here:
                owner = flip(owner, bit_of(k, stage))
            copies.append(pltpu.make_async_remote_copy(
                src_ref=rows.at[k, owner],
                dst_ref=rows.at[k, owner],
                send_sem=xs_sem.at[k, slot],
                recv_sem=xr_sem.at[k, slot],
                device_id={"seq": flip(me, bit_of(k, stage))},
            ))
        return copies

    def x_start(k, stage):
        for mine in x_copies(k, stage, True):
            mine.start()

    def x_take(k, stage):
        for theirs in x_copies(k, stage, False):
            theirs.wait_recv()

    hit = jnp.zeros((1, row_count), F32)
    for i in range(ids_ref.shape[0]):
        hit = jnp.maximum(hit, jnp.where(ids_ref[i : i + 1, :] == z, 1.0, 0.0))
    row_id = lax.broadcasted_iota(jnp.int32, (row_count, row_count), 0)
    col_id = lax.broadcasted_iota(jnp.int32, (row_count, row_count), 1)
    same = jnp.logical_and(row_id // tok == col_id // tok, row_id < col_id)
    before = dot(jnp.broadcast_to(hit, (16, row_count)).astype(BF), jnp.where(same, 1.0, 0.0).astype(BF))
    group = lax.broadcasted_iota(jnp.int32, (1, row_count), 1) // tok
    place = before[0:1].astype(jnp.int32) * n_exp + group
    place = jnp.where(hit > 0.5, place, -1)
    chosen = lax.broadcasted_iota(jnp.int32, (shard, row_count), 0) == place
    pick[...] = jnp.where(chosen, 1.0, 0.0).astype(BF)

    tri = jnp.where(row_id <= col_id, 1.0, 0.0)
    cum = dot(decay_ref[...], tri, precision=highest)
    cum_ref[...] = cum
    cum_t[...] = jnp.transpose(cum)
    step_t[...] = jnp.transpose(step_ref[...])
    b_t[...] = jnp.transpose(b_ref[...])
    keep = lax.broadcasted_iota(jnp.int32, (block, block), 1) >= lax.broadcasted_iota(
        jnp.int32, (block, block), 0
    )
    for i in range(blocks):
        span = slice(i * block, (i + 1) * block)
        cross = dot(b_t[span, :], c_ref[:, span], precision=highest)
        bc[i] = jnp.where(keep, cross, 0.0)

    inner[...] = jnp.zeros_like(inner)
    acc[...] = jnp.zeros_like(acc)
    down_copy.wait()
    hid_copy.wait()

    group_count = hid.shape[1]
    span_c = max(c for c in range(1, cap + 1) if cap % c == 0 and c * group_count <= 384)
    parts_c = cap // span_c

    def project(i):
        span = pl.ds(i * span_c, span_c)
        saved = hid[span].reshape(span_c * group_count, hid.shape[2])
        for k in range(chunks):
            part = dot(saved, down[:, k * width : (k + 1) * width])
            y_ref[k, span] = part.reshape(span_c, group_count, width)

    def z_step(i, _):
        k, d = i // steps, i % steps + 1

        @pl.when(jnp.logical_and(d == 1, k < parts_c))
        def _():
            project(k)

        @pl.when(jnp.logical_and(d == 1, k >= 2))
        def _():
            x_take(k - 2, 1)
            x_start(k - 2, 2)

        @pl.when(jnp.logical_and(d == 2, k >= 1))
        def _():
            x_take(k - 1, 0)
            x_start(k - 1, 1)

        z_take(k, d)

        @pl.when(d < steps)
        def _():
            z_send(k, d)

        @pl.when(d == steps)
        def _():
            block_in = gath[k].reshape(row_count, width)
            rows[k, me] = dot(pick[...], block_in).astype(BF)
            x_start(k, 0)
            pltpu.make_async_copy(
                proj_hbm.at[:, pl.ds(0, width)], proj.at[k], proj_sem.at[k]
            ).wait()
            inner[...] += dot(block_in, proj[k], ((1,), (1,)))

        return 0

    lax.fori_loop(0, chunks * steps, z_step, 0)
    for i in range(chunks, parts_c):
        project(i)

    left_of = lax.broadcasted_iota(jnp.int32, (1, lane), 1) < HEAD

    def pair_step(j, _):
        span = pl.ds(pl.multiple_of(j * lane, lane), lane)
        cols = [column(cum_t[...], 2 * j + i) for i in range(2)]
        rowv = [cum_ref[pl.ds(2 * j + i, 1), :] for i in range(2)]
        steps_col = jnp.where(
            left_of, column(step_t[...], 2 * j), column(step_t[...], 2 * j + 1)
        )
        col = jnp.where(left_of, cols[0], cols[1])
        end_row = jnp.where(left_of, cols[0][row_count - 1 :], cols[1][row_count - 1 :])
        fac[:, span] = steps_col * jnp.exp(end_row - col)
        skip = skip_ref[:, span]
        state = jnp.zeros((b_t.shape[1], lane), F32)
        for i in reversed(range(blocks)):
            lo, hi = i * block, (i + 1) * block
            g = inner[lo:hi, span]
            g_top, g_low = halves(g)
            both = jnp.concatenate([g_top, g_low], axis=1)
            parts, sums = [], []
            for q in range(2):
                r = rowv[q][:, lo:hi]
                w = jnp.exp(jnp.minimum(r - cols[q][lo:hi], 0.0)) * bc[i]
                w_top, w_low = halves(w)
                x = dot(w_top, both)
                parts.append(x[:, :lane] + x[:, lane:] + dot(w_low, g_top))
                base = rowv[q][:, lo - 1 : lo] if i else jnp.zeros((1, 1), F32)
                m_top, m_low = halves(c_ref[:, lo:hi] * jnp.exp(r - base))
                x = dot(m_top, both)
                sums.append(x[:, :lane] + x[:, lane:] + dot(m_low, g_top))
            result = jnp.where(left_of, parts[0], parts[1])
            if i < blocks - 1:
                edge = col[hi - 1 : hi]
                result += jnp.exp(edge - col[lo:hi]) * dot(b_t[lo:hi, :], state, precision=highest)
            start = col[lo - 1 : lo] if i else jnp.zeros((1, lane), F32)
            state = jnp.where(left_of, sums[0], sums[1]) + jnp.exp(col[hi - 1 : hi] - start) * state
            inner[lo:hi, span] = steps_col[lo:hi] * result + skip * g
        agg[0, : b_t.shape[1], span] = state
        agg[0, b_t.shape[1] :, span] = jnp.broadcast_to(end_row, (8, lane))
        return 0

    low_half = lax.broadcasted_iota(jnp.int32, (1, spread, width), 1) < n_exp

    def scores(k):
        def one(p, _):
            first = rows[k, 2 * p][: cap * n_exp].astype(F32).reshape(cap // 2, spread, width)
            second = rows[k, 2 * p + 1][: cap * n_exp].astype(F32).reshape(cap // 2, spread, width)
            even = jnp.where(low_half, first, pltpu.roll(second, n_exp, 1))
            odd = jnp.where(low_half, pltpu.roll(first, n_exp, 1), second)
            y = y_ref[k, :, pl.ds(pl.multiple_of(p * spread, spread), spread), :]
            y = y.reshape(cap // 2, 2, spread, width)
            for i, part in enumerate((even * y[:, 0], odd * y[:, 1])):
                total = part[:, :, :128]
                for j in range(1, width // 128):
                    total = total + part[:, :, j * 128 : (j + 1) * 128]
                acc[p, :, i] += total
            return 0

        lax.fori_loop(0, n_seq // 2, one, 0)

    tasks = []
    for stage in range(1, n_stage + 1):
        for k in range(chunks):
            if k + stage >= chunks:
                tasks.append((k, stage))
    tasks.sort(key=lambda t: (t[0] + 1.5 * t[1], t[0]))

    def serve(count):
        for _ in range(min(count, len(tasks))):
            k, stage = tasks.pop(0)
            x_take(k, stage - 1)
            x_start(k, stage)

    cut = pairs // 2
    lax.fori_loop(0, cut, pair_step, 0)
    serve(1)
    lax.fori_loop(cut, pairs, pair_step, 0)

    n_state = b_t.shape[1]
    carry[...] = jnp.zeros_like(carry)
    reach = jnp.zeros((1, channels), F32)

    def a_copy(i, bit):
        return pltpu.make_async_remote_copy(
            src_ref=agg.at[i],
            dst_ref=got.at[i],
            send_sem=as_sem.at[i],
            recv_sem=ar_sem.at[i],
            device_id={"seq": flip(me, bit)},
        )

    order = [1] + bits
    a_copy(0, 1).start()
    for i, bit in enumerate(order):
        if i == 0:
            serve(1)
        x_take(i, n_stage)
        scores(i)
        a_copy(i, bit).wait_recv()
        low = ((me // bit) % 2) == 0
        other, other_t = got[i, :n_state, :], got[i, n_state : n_state + 1, :]
        own, own_t = agg[i, :n_state, :], agg[i, n_state : n_state + 1, :]
        carry[...] += jnp.where(low, jnp.exp(reach) * other, 0.0)
        reach = reach + jnp.where(low, other_t, 0.0)
        if i + 1 < len(order):
            first = jnp.where(low, own, other)
            first_t = jnp.where(low, own_t, other_t)
            second = jnp.where(low, other, own)
            agg[i + 1, :n_state, :] = first + jnp.exp(first_t) * second
            agg[i + 1, n_state:, :] = jnp.broadcast_to(own_t + other_t, (8, channels))
            a_copy(i + 1, order[i + 1]).start()

    for i in range(blocks):
        lo, hi = i * block, (i + 1) * block
        from_carry = dot(b_t[lo:hi, :], carry[...], precision=highest)
        out_ref[lo:hi, :] = (inner[lo:hi, :] + fac[lo:hi, :] * from_carry).astype(BF)

    for k in range(len(order), chunks):
        if k == chunks - 2:
            serve(len(tasks))
        x_take(k, n_stage)
        scores(k)

    def finish(p, _):
        wide = jnp.transpose(acc[p].reshape(cap * spread, 128))
        mail[p] = jnp.sum(wide, axis=0, keepdims=True)
        return 0

    lax.fori_loop(0, n_seq // 2, finish, 0)

    def mail_copy(other, source, slot):
        return pltpu.make_async_remote_copy(
            src_ref=mail.at[other // spread],
            dst_ref=inbox.at[source],
            send_sem=ms_sem.at[slot],
            recv_sem=mr_sem.at[source],
            device_id={"seq": other // n_exp, "exp": lax.rem(other, n_exp)},
        )

    def post(i, _):
        other = lax.rem(mine_id + i, n_dev)
        mail_copy(other, mine_id, other).start()
        return 0

    def take(i, _):
        other = lax.rem(mine_id + i, n_dev)
        mail_copy(other, other, other).wait_recv()
        return 0

    def posted(i, _):
        other = lax.rem(mine_id + i, n_dev)
        mail_copy(other, mine_id, other).wait_send()
        return 0

    lax.fori_loop(1, n_dev, post, 0)
    inbox[mine_id] = mail[me // 2]
    lax.fori_loop(1, n_dev, take, 0)
    for e in range(n_exp):
        total = inbox[e]
        for i in range(1, n_seq):
            total = total + inbox[i * n_exp + e]
        table_ref[e] = total
    lax.fori_loop(1, n_dev, posted, 0)

    for k in range(chunks):
        for d in range(steps):
            z_sent(k, d)
        for stage in range(n_stage + 1):
            for mine in x_copies(k, stage, True):
                mine.wait_send()
    for i, bit in enumerate(order):
        a_copy(i, bit).wait_send()


def plan(n_seq, n_exp, tok, depth, channels, cap, hidden, state):
    chunks = 8
    width = depth // chunks
    shard = -(-cap * n_exp // 16) * 16
    row_count = n_exp * tok
    letter = cap * n_exp * 2
    block = min(256, row_count)
    heads = channels // HEAD
    stages = n_seq.bit_length() - 1
    steps = n_exp - 1
    shapes = [
        ((chunks, n_exp, tok, width), BF),
        ((chunks, channels, width), BF),
        ((cap, n_seq * n_exp, hidden), BF),
        ((hidden, depth), BF),
        ((chunks, cap, n_seq * n_exp, width), F32),
        ((chunks, n_seq, shard, width), BF),
        ((shard, row_count), BF),
        ((row_count, channels), F32),
        ((row_count, channels), F32),
        ((n_seq // 2, cap // 2, 2, 2 * n_exp, 128), F32),
        ((heads, row_count), F32),
        ((row_count, heads), F32),
        ((row_count, heads), F32),
        ((row_count, state), F32),
        ((row_count // block, block, block), F32),
        ((stages, state + 8, channels), F32),
        ((stages, state + 8, channels), F32),
        ((state, channels), F32),
        ((n_seq // 2, 1, letter), F32),
        ((n_seq * n_exp, 1, letter), F32),
    ]
    total = 0
    for shape, kind in shapes:
        size = 1
        for extent in shape:
            size *= extent
        total += size * (2 if kind is BF else 4)
    fits = (
        total < VMEM_ROOM - (8 << 20)
        and n_seq & (n_seq - 1) == 0
        and stages == 3
        and n_exp == 4
        and cap % 2 == 0
        and depth % (128 * chunks) == 0
        and channels % (2 * HEAD) == 0
        and row_count % block == 0
        and tok % 8 == 0
    )
    sems = [
        (chunks,), (), (), (chunks,),
        (2, chunks, steps), (2, chunks, steps),
        (chunks, n_seq - 1), (chunks, n_seq - 1),
        (stages,), (stages,),
        (n_seq * n_exp,), (n_seq * n_exp,),
    ]
    return fits, (n_seq, n_exp, tok, cap, shard, chunks, width), shapes, sems


def quick(
    fitted, grad_out, out_proj, step_size, log_decay, b_input, c_output, skip_gain, expert_ids,
    hidden_act, w_down,
):
    _, sizes, shapes, sems = fitted
    n_seq, n_exp, tok, cap, shard, chunks, width = sizes
    vmem = pl.BlockSpec(memory_space=pltpu.VMEM)
    hbm = pl.BlockSpec(memory_space=pl.ANY)
    row_count, channels = n_exp * tok, out_proj.shape[0]
    d_inner, table = pl.pallas_call(
        functools.partial(fused, sizes),
        out_shape=(
            jax.ShapeDtypeStruct((row_count, channels), BF),
            jax.ShapeDtypeStruct((n_exp, 1, 2 * n_exp * cap), F32),
        ),
        in_specs=[hbm] * 4 + [vmem] * 6,
        out_specs=(vmem, vmem),
        scratch_shapes=[pltpu.VMEM(shape, kind) for shape, kind in shapes]
        + [pltpu.SemaphoreType.DMA(s) if s else pltpu.SemaphoreType.DMA for s in sems],
        compiler_params=pltpu.CompilerParams(
            collective_id=0, has_side_effects=True, vmem_limit_bytes=VMEM_ROOM
        ),
    )(
        grad_out, out_proj, hidden_act.transpose(0, 2, 1, 3), w_down, step_size, log_decay, b_input, c_output,
        skip_gain.reshape(1, -1), expert_ids.T,
    )
    exp_index = lax.axis_index("exp")
    own_ids = lax.dynamic_slice_in_dim(expert_ids, exp_index * tok, tok, 0)
    group = lax.rem(lax.axis_index("seq"), 2) * n_exp + exp_index
    experts = lax.broadcasted_iota(jnp.int32, (1, 1, n_exp), 2)
    onehot = own_ids[:, :, None] == experts
    member = jnp.any(onehot, axis=1).astype(jnp.int32)
    rank_ids = jnp.cumsum(member, axis=0) - 1
    slot_of = jnp.sum(jnp.where(onehot, rank_ids[:, None, :], 0), axis=2)
    spot = own_ids * table.shape[2] + slot_of * (2 * n_exp) + group
    flat = table.reshape(1, 1, -1)
    spots = lax.broadcasted_iota(jnp.int32, flat.shape, 2)
    d_gate = jnp.sum(jnp.where(spots == spot.T[:, :, None], flat, 0.0), axis=2)
    return d_inner, d_gate


def route(*args):
    grad_out, out_proj, step_size, log_decay, b_input, c_output, skip_gain, ids, hidden, down = args
    fitted = plan(
        lax.axis_size("seq"), lax.axis_size("exp"), grad_out.shape[0], grad_out.shape[1],
        out_proj.shape[0], hidden.shape[2], hidden.shape[3], b_input.shape[0],
    )
    if fitted[0]:
        return quick(fitted, *args)
    return shards(*args)


def solution(mesh):
    in_specs = (
        P(("seq", "exp"), None),
        P("exp", None),
        P("exp", "seq"),
        P("exp", "seq"),
        P(None, "seq"),
        P(None, "seq"),
        P("exp"),
        P("seq", None),
        P("exp", None, None, "seq"),
        P("exp", "seq", None),
    )
    out_specs = (P("seq", "exp"), P(None, ("seq", "exp")))
    return jax.shard_map(route, mesh=mesh, in_specs=in_specs, out_specs=out_specs, check_vma=False)
```

```python
import functools

import jax
import jax.numpy as jnp
from jax import lax
from jax.experimental import pallas as pl
from jax.experimental.pallas import tpu as pltpu
from jax.sharding import PartitionSpec as P

HEAD = 64


highest = lax.Precision.HIGHEST


def block_pass(state_in, pieces):
    grad_block, decay_block, step_block, b_block, c_block = pieces
    cum_decay = jnp.cumsum(decay_block, axis=1)
    gap_table = cum_decay[:, None, :] - cum_decay[:, :, None]
    upper_mask = lax.broadcasted_iota(jnp.int32, gap_table.shape, 2) >= lax.broadcasted_iota(
        jnp.int32, gap_table.shape, 1
    )
    weights = jnp.where(upper_mask, jnp.exp(jnp.where(upper_mask, gap_table, 0.0)), 0.0)
    intersection = lax.dot_general(
        b_block,
        c_block,
        (((0,), (0,)), ((), ())),
        precision=highest,
        preferred_element_type=jnp.float32,
    )
    within = jnp.einsum("hut,thp->uhp", weights * intersection[None], grad_block, precision=highest)
    tail_decay = jnp.exp(cum_decay[:, -1:] - cum_decay)
    from_state = (
        jnp.einsum("nu,hnp->uhp", b_block, state_in, precision=highest) * tail_decay.T[:, :, None]
    )
    result = step_block.T[:, :, None] * (within + from_state)
    state_out = jnp.einsum(
        "ht,nt,thp->hnp", jnp.exp(cum_decay), c_block, grad_block, precision=highest
    )
    state_out = state_out + jnp.exp(cum_decay[:, -1])[:, None, None] * state_in
    return (state_out, result)


def local_sweep(grad_rows, decay_rows, step_rows, b_rows, c_rows, start_state):
    row_count = grad_rows.shape[0]
    head_count = decay_rows.shape[0]
    block_len = min(512, row_count)
    block_count = row_count // block_len
    pieces = (
        grad_rows.reshape(block_count, block_len, head_count, grad_rows.shape[2]),
        decay_rows.reshape(head_count, block_count, block_len).transpose(1, 0, 2),
        step_rows.reshape(head_count, block_count, block_len).transpose(1, 0, 2),
        b_rows.reshape(b_rows.shape[0], block_count, block_len).transpose(1, 0, 2),
        c_rows.reshape(c_rows.shape[0], block_count, block_len).transpose(1, 0, 2),
    )
    state_out, results = lax.scan(block_pass, start_state, pieces, reverse=True)
    return (state_out, results.reshape(row_count, head_count, grad_rows.shape[2]))


def route_table(groups, expert, cap_len):
    hit_mask = jnp.any(groups == expert, axis=2)
    rank_ids = jnp.cumsum(hit_mask.astype(jnp.int32), axis=1) - 1
    slot_ids = lax.broadcasted_iota(jnp.int32, (1, 1, cap_len), 2)
    chosen = jnp.logical_and(hit_mask[:, :, None], rank_ids[:, :, None] == slot_ids)
    token_ids = lax.broadcasted_iota(jnp.int32, chosen.shape, 1)
    position = jnp.sum(jnp.where(chosen, token_ids, 0), axis=1)
    filled = jnp.any(chosen, axis=1)
    return (position, filled)


def slot_lookup(slot_table, own_ids, cap_len, expert_count):
    experts_iota = lax.broadcasted_iota(jnp.int32, (1, 1, expert_count), 2)
    onehot = own_ids[:, :, None] == experts_iota
    member = jnp.any(onehot, axis=1).astype(jnp.int32)
    rank_ids = jnp.cumsum(member, axis=0) - 1
    slot_of = jnp.sum(jnp.where(onehot, rank_ids[:, None, :], 0), axis=2)
    picked = jnp.sum(jnp.where(onehot[:, :, :, None], slot_table[None, None], 0.0), axis=2)
    slot_iota = lax.broadcasted_iota(jnp.int32, (1, 1, cap_len), 2)
    return jnp.sum(jnp.where(slot_of[:, :, None] == slot_iota, picked, 0.0), axis=2)


def shards(
    grad_out,
    out_proj,
    step_size,
    log_decay,
    b_input,
    c_output,
    skip_gain,
    expert_ids,
    hidden_act,
    w_down,
):
    exp_index = lax.axis_index("exp")
    seq_index = lax.axis_index("seq")
    exp_count = lax.axis_size("exp")
    seq_count = lax.axis_size("seq")
    tok_len = grad_out.shape[0]
    cap_len = hidden_act.shape[2]
    gathered = lax.all_gather(grad_out, "exp", axis=0, tiled=True)
    groups = expert_ids.reshape(exp_count, tok_len, expert_ids.shape[1])
    position, filled = route_table(groups, exp_index, cap_len)
    flat_index = (position + lax.broadcasted_iota(jnp.int32, position.shape, 0) * tok_len).reshape(
        -1
    )
    slot_rows = jnp.take(gathered, flat_index, axis=0)
    slot_rows = jnp.where(filled.reshape(-1, 1), slot_rows, jnp.zeros_like(slot_rows))
    saved_rows = hidden_act.reshape(-1, hidden_act.shape[3])
    weights = w_down[0]
    projected = lax.dot_general(
        lax.all_gather(slot_rows, "seq", axis=0, tiled=True),
        weights,
        (((1,), (1,)), ((), ())),
        preferred_element_type=jnp.float32,
    )
    partial_scores = jnp.sum(projected * saved_rows.astype(jnp.float32), axis=1)
    head_count = out_proj.shape[0] // HEAD
    inner_grad = lax.dot_general(
        gathered, out_proj, (((1,), (1,)), ((), ())), preferred_element_type=jnp.float32
    )
    row_count = inner_grad.shape[0]
    start_state = jnp.zeros((head_count, b_input.shape[0], HEAD), jnp.float32)
    summary, swept_part = local_sweep(
        inner_grad.reshape(row_count, head_count, HEAD),
        log_decay,
        step_size,
        b_input,
        c_output,
        start_state,
    )
    total_decay = jnp.sum(log_decay, axis=1)
    all_states, all_decay = (
        lax.all_gather(summary[None], "seq", axis=0, tiled=True),
        lax.all_gather(total_decay[None], "seq", axis=0, tiled=True),
    )
    shard_ids = lax.broadcasted_iota(jnp.int32, all_decay.shape, 0)
    beyond = jnp.where(shard_ids > seq_index, all_decay, 0.0)
    exponent = jnp.cumsum(beyond, axis=0) - beyond
    factor = jnp.where(
        shard_ids > seq_index, jnp.exp(jnp.where(shard_ids > seq_index, exponent, 0.0)), 0.0
    )
    incoming = jnp.sum(factor[:, :, None, None] * all_states, axis=0)
    suffix = jnp.flip(jnp.cumsum(jnp.flip(log_decay, 1), axis=1), 1) - log_decay
    from_carry = (
        jnp.einsum("nu,hnp->uhp", b_input, incoming, precision=highest)
        * jnp.exp(suffix).T[:, :, None]
    )
    combined = swept_part + step_size.T[:, :, None] * from_carry
    d_inner = (combined.reshape(row_count, -1) + skip_gain * inner_grad).astype(jnp.bfloat16)
    summed = lax.psum_scatter(
        partial_scores.reshape(seq_count, exp_count, cap_len),
        "seq",
        scatter_dimension=0,
        tiled=True,
    )
    slot_table = lax.all_to_all(
        summed.reshape(exp_count, 1, cap_len), "exp", split_axis=0, concat_axis=1, tiled=True
    ).reshape(exp_count, cap_len)
    own_ids = lax.dynamic_slice_in_dim(expert_ids, exp_index * tok_len, tok_len, 0)
    d_gate = slot_lookup(slot_table, own_ids, cap_len, exp_count).T
    return (d_inner, d_gate)


VMEM_ROOM = 60 << 20
BF = jnp.bfloat16
F32 = jnp.float32


def halves(x):
    top = x.astype(BF)
    return top, (x - top.astype(F32)).astype(BF)


def dot(x, y, dims=((1,), (0,)), precision=None):
    return lax.dot_general(x, y, (dims, ((), ())), precision=precision, preferred_element_type=F32)


def flip(index, bit):
    return index + bit - 2 * bit * ((index // bit) % 2)


def column(table, h):
    lanes = lax.broadcasted_iota(jnp.int32, table.shape, 1)
    return jnp.sum(jnp.where(lanes == h, table, 0.0), axis=1, keepdims=True)


def fused(
    sizes,
    grad_hbm, proj_hbm, hid_hbm, down_hbm, step_ref, decay_ref, b_ref, c_ref, skip_ref, ids_ref,
    out_ref, table_ref,
    gath, proj, hid, down, y_ref, rows, pick, inner, fac, acc,
    cum_ref, cum_t, step_t, b_t, bc, agg, got, carry, mail, inbox,
    load_sem, hid_sem, down_sem, proj_sem,
    zs_sem, zr_sem, xs_sem, xr_sem, as_sem, ar_sem, ms_sem, mr_sem,
):
    n_seq, n_exp, tok, cap, shard, chunks, width = sizes
    me = lax.axis_index("seq")
    z = lax.axis_index("exp")
    row_count = n_exp * tok
    spread = 2 * n_exp
    n_dev = n_seq * n_exp
    mine_id = me * n_exp + z
    bits = [1 << i for i in range(1, n_seq.bit_length() - 1)]
    n_stage = len(bits)
    steps = n_exp - 1
    block = bc.shape[1]
    blocks = row_count // block
    channels = inner.shape[1]
    lane = 2 * HEAD
    pairs = channels // lane

    for k in range(chunks):
        pltpu.make_async_copy(
            grad_hbm.at[:, pl.ds(k * width, width)], gath.at[k, z], load_sem.at[k]
        ).start()
    down_copy = pltpu.make_async_copy(down_hbm.at[0], down, down_sem)
    down_copy.start()
    hid_copy = pltpu.make_async_copy(hid_hbm.at[0], hid, hid_sem)
    hid_copy.start()
    for k in range(chunks):
        pltpu.make_async_copy(
            proj_hbm.at[:, pl.ds(k * width, width)], proj.at[k], proj_sem.at[k]
        ).start()

    barrier = pltpu.get_barrier_semaphore()

    def greet(i, _):
        other = lax.rem(mine_id + i, n_dev)
        pl.semaphore_signal(
            barrier, inc=1, device_id={"seq": other // n_exp, "exp": lax.rem(other, n_exp)}
        )
        return 0

    lax.fori_loop(1, n_dev, greet, 0)
    pl.semaphore_wait(barrier, n_dev - 1)

    def z_copy(side, k, d, owner, target):
        return pltpu.make_async_remote_copy(
            src_ref=gath.at[k, owner],
            dst_ref=gath.at[k, owner],
            send_sem=zs_sem.at[side, k, d],
            recv_sem=zr_sem.at[side, k, d],
            device_id={"exp": target},
        )

    def z_send(k, d):
        @pl.when(jnp.logical_and(z < n_exp - 1, z - d >= 0))
        def _():
            z_copy(0, k, d, z - d, z + 1).start()

        @pl.when(jnp.logical_and(z > 0, z + d < n_exp))
        def _():
            z_copy(1, k, d, z + d, z - 1).start()

    def z_sent(k, d):
        @pl.when(jnp.logical_and(z < n_exp - 1, z - d >= 0))
        def _():
            z_copy(0, k, d, z - d, z + 1).wait_send()

        @pl.when(jnp.logical_and(z > 0, z + d < n_exp))
        def _():
            z_copy(1, k, d, z + d, z - 1).wait_send()

    def z_take(k, d):
        @pl.when(z - d >= 0)
        def _():
            z_copy(0, k, d - 1, z - d, z).wait_recv()

        @pl.when(z + d < n_exp)
        def _():
            z_copy(1, k, d - 1, z + d, z).wait_recv()

    for k in range(chunks):
        pltpu.make_async_copy(
            grad_hbm.at[:, pl.ds(k * width, width)], gath.at[k, z], load_sem.at[k]
        ).wait()
        if k == 0:
            z_send(k, 0)

    def bit_of(k, stage):
        if stage == n_stage:
            return 1
        low, high = bits[stage], bits[n_stage - 1 - stage]
        return low + (high - low) * (k % 2)

    def x_copies(k, stage, here):
        masks = [()]
        for i in range(stage):
            masks = masks + [m + (i,) for m in masks]
        copies = []
        for j, mask in enumerate(masks):
            owner = me
            for i in mask:
                owner = flip(owner, bit_of(k, i))
            slot = (1 << stage) - 1 + j
            if not here:
                owner = flip(owner, bit_of(k, stage))
            copies.append(pltpu.make_async_remote_copy(
                src_ref=rows.at[k, owner],
                dst_ref=rows.at[k, owner],
                send_sem=xs_sem.at[k, slot],
                recv_sem=xr_sem.at[k, slot],
                device_id={"seq": flip(me, bit_of(k, stage))},
            ))
        return copies

    def x_start(k, stage):
        for mine in x_copies(k, stage, True):
            mine.start()

    def x_take(k, stage):
        for theirs in x_copies(k, stage, False):
            theirs.wait_recv()

    hit = jnp.zeros((1, row_count), F32)
    for i in range(ids_ref.shape[0]):
        hit = jnp.maximum(hit, jnp.where(ids_ref[i : i + 1, :] == z, 1.0, 0.0))
    row_id = lax.broadcasted_iota(jnp.int32, (row_count, row_count), 0)
    col_id = lax.broadcasted_iota(jnp.int32, (row_count, row_count), 1)
    same = jnp.logical_and(row_id // tok == col_id // tok, row_id < col_id)
    before = dot(jnp.broadcast_to(hit, (16, row_count)).astype(BF), jnp.where(same, 1.0, 0.0).astype(BF))
    group = lax.broadcasted_iota(jnp.int32, (1, row_count), 1) // tok
    place = before[0:1].astype(jnp.int32) * n_exp + group
    place = jnp.where(hit > 0.5, place, -1)
    chosen = lax.broadcasted_iota(jnp.int32, (shard, row_count), 0) == place
    pick[...] = jnp.where(chosen, 1.0, 0.0).astype(BF)

    tri = jnp.where(row_id <= col_id, 1.0, 0.0)
    cum = dot(decay_ref[...], tri, precision=highest)
    cum_ref[...] = cum
    cum_t[...] = jnp.transpose(cum)
    step_t[...] = jnp.transpose(step_ref[...])
    b_t[...] = jnp.transpose(b_ref[...])
    keep = lax.broadcasted_iota(jnp.int32, (block, block), 1) >= lax.broadcasted_iota(
        jnp.int32, (block, block), 0
    )
    for i in range(blocks):
        span = slice(i * block, (i + 1) * block)
        cross = dot(b_t[span, :], c_ref[:, span], precision=highest)
        bc[i] = jnp.where(keep, cross, 0.0)

    inner[...] = jnp.zeros_like(inner)
    acc[...] = jnp.zeros_like(acc)
    down_copy.wait()
    hid_copy.wait()

    group_count = hid.shape[1]
    span_c = max(c for c in range(1, cap + 1) if cap % c == 0 and c * group_count <= 384)
    parts_c = cap // span_c

    def project(i):
        span = pl.ds(i * span_c, span_c)
        saved = hid[span].reshape(span_c * group_count, hid.shape[2])
        for k in range(chunks):
            part = dot(saved, down[:, k * width : (k + 1) * width])
            y_ref[k, span] = part.reshape(span_c, group_count, width)

    def z_step(i, _):
        k, d = i // steps, i % steps + 1
        z_take(k, d)

        @pl.when(d < steps)
        def _():
            z_send(k, d)

        @pl.when(jnp.logical_and(d == 1, k < chunks - 1))
        def _():
            z_send(k + 1, 0)

        @pl.when(jnp.logical_and(d == 1, k >= 2))
        def _():
            x_take(k - 2, 1)
            x_start(k - 2, 2)

        @pl.when(jnp.logical_and(d == 2, k >= 1))
        def _():
            x_take(k - 1, 0)
            x_start(k - 1, 1)

        @pl.when(jnp.logical_and(d == 1, k < parts_c))
        def _():
            project(k)

        @pl.when(d == steps)
        def _():
            block_in = gath[k].reshape(row_count, width)
            rows[k, me] = dot(pick[...], block_in).astype(BF)
            x_start(k, 0)
            pltpu.make_async_copy(
                proj_hbm.at[:, pl.ds(0, width)], proj.at[k], proj_sem.at[k]
            ).wait()
            inner[...] += dot(block_in, proj[k], ((1,), (1,)))

        return 0

    lax.fori_loop(0, chunks * steps, z_step, 0)
    for i in range(chunks, parts_c):
        project(i)

    left_of = lax.broadcasted_iota(jnp.int32, (1, lane), 1) < HEAD

    def pair_step(j, _):
        span = pl.ds(pl.multiple_of(j * lane, lane), lane)
        cols = [column(cum_t[...], 2 * j + i) for i in range(2)]
        rowv = [cum_ref[pl.ds(2 * j + i, 1), :] for i in range(2)]
        steps_col = jnp.where(
            left_of, column(step_t[...], 2 * j), column(step_t[...], 2 * j + 1)
        )
        col = jnp.where(left_of, cols[0], cols[1])
        end_row = jnp.where(left_of, cols[0][row_count - 1 :], cols[1][row_count - 1 :])
        fac[:, span] = steps_col * jnp.exp(end_row - col)
        skip = skip_ref[:, span]
        state = jnp.zeros((b_t.shape[1], lane), F32)
        for i in reversed(range(blocks)):
            lo, hi = i * block, (i + 1) * block
            g = inner[lo:hi, span]
            g_top, g_low = halves(g)
            both = jnp.concatenate([g_top, g_low], axis=1)
            parts, sums = [], []
            for q in range(2):
                r = rowv[q][:, lo:hi]
                w = jnp.exp(jnp.minimum(r - cols[q][lo:hi], 0.0)) * bc[i]
                w_top, w_low = halves(w)
                x = dot(w_top, both)
                parts.append(x[:, :lane] + x[:, lane:] + dot(w_low, g_top))
                base = rowv[q][:, lo - 1 : lo] if i else jnp.zeros((1, 1), F32)
                m_top, m_low = halves(c_ref[:, lo:hi] * jnp.exp(r - base))
                x = dot(m_top, both)
                sums.append(x[:, :lane] + x[:, lane:] + dot(m_low, g_top))
            result = jnp.where(left_of, parts[0], parts[1])
            if i < blocks - 1:
                edge = col[hi - 1 : hi]
                result += jnp.exp(edge - col[lo:hi]) * dot(b_t[lo:hi, :], state, precision=highest)
            start = col[lo - 1 : lo] if i else jnp.zeros((1, lane), F32)
            state = jnp.where(left_of, sums[0], sums[1]) + jnp.exp(col[hi - 1 : hi] - start) * state
            inner[lo:hi, span] = steps_col[lo:hi] * result + skip * g
        agg[0, : b_t.shape[1], span] = state
        agg[0, b_t.shape[1] :, span] = jnp.broadcast_to(end_row, (8, lane))
        return 0

    low_half = lax.broadcasted_iota(jnp.int32, (1, spread, width), 1) < n_exp

    def scores(k):
        def one(p, _):
            first = rows[k, 2 * p][: cap * n_exp].astype(F32).reshape(cap // 2, spread, width)
            second = rows[k, 2 * p + 1][: cap * n_exp].astype(F32).reshape(cap // 2, spread, width)
            even = jnp.where(low_half, first, pltpu.roll(second, n_exp, 1))
            odd = jnp.where(low_half, pltpu.roll(first, n_exp, 1), second)
            y = y_ref[k, :, pl.ds(pl.multiple_of(p * spread, spread), spread), :]
            y = y.reshape(cap // 2, 2, spread, width)
            for i, part in enumerate((even * y[:, 0], odd * y[:, 1])):
                total = part[:, :, :128]
                for j in range(1, width // 128):
                    total = total + part[:, :, j * 128 : (j + 1) * 128]
                acc[p, :, i] += total
            return 0

        lax.fori_loop(0, n_seq // 2, one, 0)

    tasks = []
    for stage in range(1, n_stage + 1):
        for k in range(chunks):
            if k + stage >= chunks:
                tasks.append((k, stage))
    tasks.sort(key=lambda t: (t[0] + 1.5 * t[1], t[0]))

    def serve(count):
        for _ in range(min(count, len(tasks))):
            k, stage = tasks.pop(0)
            x_take(k, stage - 1)
            x_start(k, stage)

    cut = pairs // 2
    lax.fori_loop(0, cut, pair_step, 0)
    serve(1)
    lax.fori_loop(cut, pairs, pair_step, 0)

    n_state = b_t.shape[1]
    carry[...] = jnp.zeros_like(carry)
    reach = jnp.zeros((1, channels), F32)

    def a_copy(i, bit):
        return pltpu.make_async_remote_copy(
            src_ref=agg.at[i],
            dst_ref=got.at[i],
            send_sem=as_sem.at[i],
            recv_sem=ar_sem.at[i],
            device_id={"seq": flip(me, bit)},
        )

    order = [1] + bits
    a_copy(0, 1).start()
    for i, bit in enumerate(order):
        if i == 0:
            serve(1)
        while (i, n_stage) in tasks:
            serve(1)
        x_take(i, n_stage)
        scores(i)
        a_copy(i, bit).wait_recv()
        low = ((me // bit) % 2) == 0
        other, other_t = got[i, :n_state, :], got[i, n_state : n_state + 1, :]
        own, own_t = agg[i, :n_state, :], agg[i, n_state : n_state + 1, :]
        carry[...] += jnp.where(low, jnp.exp(reach) * other, 0.0)
        reach = reach + jnp.where(low, other_t, 0.0)
        if i + 1 < len(order):
            first = jnp.where(low, own, other)
            first_t = jnp.where(low, own_t, other_t)
            second = jnp.where(low, other, own)
            agg[i + 1, :n_state, :] = first + jnp.exp(first_t) * second
            agg[i + 1, n_state:, :] = jnp.broadcast_to(own_t + other_t, (8, channels))
            a_copy(i + 1, order[i + 1]).start()

    for i in range(blocks):
        lo, hi = i * block, (i + 1) * block
        from_carry = dot(b_t[lo:hi, :], carry[...], precision=highest)
        out_ref[lo:hi, :] = (inner[lo:hi, :] + fac[lo:hi, :] * from_carry).astype(BF)

    for k in range(len(order), chunks):
        if k >= chunks - 2:
            serve(len(tasks))
        x_take(k, n_stage)
        scores(k)

    def finish(p, _):
        wide = jnp.transpose(acc[p].reshape(cap * spread, 128))
        mail[p] = jnp.sum(wide, axis=0, keepdims=True)
        return 0

    lax.fori_loop(0, n_seq // 2, finish, 0)

    def mail_copy(other, source, slot):
        return pltpu.make_async_remote_copy(
            src_ref=mail.at[other // spread],
            dst_ref=inbox.at[source],
            send_sem=ms_sem.at[slot],
            recv_sem=mr_sem.at[source],
            device_id={"seq": other // n_exp, "exp": lax.rem(other, n_exp)},
        )

    def post(i, _):
        other = lax.rem(mine_id + i, n_dev)
        mail_copy(other, mine_id, other).start()
        return 0

    def take(i, _):
        other = lax.rem(mine_id + i, n_dev)
        mail_copy(other, other, other).wait_recv()
        return 0

    def posted(i, _):
        other = lax.rem(mine_id + i, n_dev)
        mail_copy(other, mine_id, other).wait_send()
        return 0

    lax.fori_loop(1, n_dev, post, 0)
    inbox[mine_id] = mail[me // 2]
    lax.fori_loop(1, n_dev, take, 0)
    for e in range(n_exp):
        total = inbox[e]
        for i in range(1, n_seq):
            total = total + inbox[i * n_exp + e]
        table_ref[e] = total
    lax.fori_loop(1, n_dev, posted, 0)

    for k in range(chunks):
        for d in range(steps):
            z_sent(k, d)
        for stage in range(n_stage + 1):
            for mine in x_copies(k, stage, True):
                mine.wait_send()
    for i, bit in enumerate(order):
        a_copy(i, bit).wait_send()


def plan(n_seq, n_exp, tok, depth, channels, cap, hidden, state):
    chunks = 8
    width = depth // chunks
    shard = -(-cap * n_exp // 16) * 16
    row_count = n_exp * tok
    letter = cap * n_exp * 2
    block = min(256, row_count)
    heads = channels // HEAD
    stages = n_seq.bit_length() - 1
    steps = n_exp - 1
    shapes = [
        ((chunks, n_exp, tok, width), BF),
        ((chunks, channels, width), BF),
        ((cap, n_seq * n_exp, hidden), BF),
        ((hidden, depth), BF),
        ((chunks, cap, n_seq * n_exp, width), F32),
        ((chunks, n_seq, shard, width), BF),
        ((shard, row_count), BF),
        ((row_count, channels), F32),
        ((row_count, channels), F32),
        ((n_seq // 2, cap // 2, 2, 2 * n_exp, 128), F32),
        ((heads, row_count), F32),
        ((row_count, heads), F32),
        ((row_count, heads), F32),
        ((row_count, state), F32),
        ((row_count // block, block, block), F32),
        ((stages, state + 8, channels), F32),
        ((stages, state + 8, channels), F32),
        ((state, channels), F32),
        ((n_seq // 2, 1, letter), F32),
        ((n_seq * n_exp, 1, letter), F32),
    ]
    total = 0
    for shape, kind in shapes:
        size = 1
        for extent in shape:
            size *= extent
        total += size * (2 if kind is BF else 4)
    fits = (
        total < VMEM_ROOM - (8 << 20)
        and n_seq & (n_seq - 1) == 0
        and stages == 3
        and n_exp == 4
        and cap % 2 == 0
        and depth % (128 * chunks) == 0
        and channels % (2 * HEAD) == 0
        and row_count % block == 0
        and tok % 8 == 0
    )
    sems = [
        (chunks,), (), (), (chunks,),
        (2, chunks, steps), (2, chunks, steps),
        (chunks, n_seq - 1), (chunks, n_seq - 1),
        (stages,), (stages,),
        (n_seq * n_exp,), (n_seq * n_exp,),
    ]
    return fits, (n_seq, n_exp, tok, cap, shard, chunks, width), shapes, sems


def quick(
    fitted, grad_out, out_proj, step_size, log_decay, b_input, c_output, skip_gain, expert_ids,
    hidden_act, w_down,
):
    _, sizes, shapes, sems = fitted
    n_seq, n_exp, tok, cap, shard, chunks, width = sizes
    vmem = pl.BlockSpec(memory_space=pltpu.VMEM)
    hbm = pl.BlockSpec(memory_space=pl.ANY)
    row_count, channels = n_exp * tok, out_proj.shape[0]
    d_inner, table = pl.pallas_call(
        functools.partial(fused, sizes),
        out_shape=(
            jax.ShapeDtypeStruct((row_count, channels), BF),
            jax.ShapeDtypeStruct((n_exp, 1, 2 * n_exp * cap), F32),
        ),
        in_specs=[hbm] * 4 + [vmem] * 6,
        out_specs=(vmem, vmem),
        scratch_shapes=[pltpu.VMEM(shape, kind) for shape, kind in shapes]
        + [pltpu.SemaphoreType.DMA(s) if s else pltpu.SemaphoreType.DMA for s in sems],
        compiler_params=pltpu.CompilerParams(
            collective_id=0, has_side_effects=True, vmem_limit_bytes=VMEM_ROOM
        ),
    )(
        grad_out, out_proj, hidden_act.transpose(0, 2, 1, 3), w_down, step_size, log_decay, b_input, c_output,
        skip_gain.reshape(1, -1), expert_ids.T,
    )
    exp_index = lax.axis_index("exp")
    own_ids = lax.dynamic_slice_in_dim(expert_ids, exp_index * tok, tok, 0)
    group = lax.rem(lax.axis_index("seq"), 2) * n_exp + exp_index
    experts = lax.broadcasted_iota(jnp.int32, (1, 1, n_exp), 2)
    onehot = own_ids[:, :, None] == experts
    member = jnp.any(onehot, axis=1).astype(jnp.int32)
    rank_ids = jnp.cumsum(member, axis=0) - 1
    slot_of = jnp.sum(jnp.where(onehot, rank_ids[:, None, :], 0), axis=2)
    spot = own_ids * table.shape[2] + slot_of * (2 * n_exp) + group
    flat = table.reshape(1, 1, -1)
    spots = lax.broadcasted_iota(jnp.int32, flat.shape, 2)
    d_gate = jnp.sum(jnp.where(spots == spot.T[:, :, None], flat, 0.0), axis=2)
    return d_inner, d_gate


def route(*args):
    grad_out, out_proj, step_size, log_decay, b_input, c_output, skip_gain, ids, hidden, down = args
    fitted = plan(
        lax.axis_size("seq"), lax.axis_size("exp"), grad_out.shape[0], grad_out.shape[1],
        out_proj.shape[0], hidden.shape[2], hidden.shape[3], b_input.shape[0],
    )
    if fitted[0]:
        return quick(fitted, *args)
    return shards(*args)


def solution(mesh):
    in_specs = (
        P(("seq", "exp"), None),
        P("exp", None),
        P("exp", "seq"),
        P("exp", "seq"),
        P(None, "seq"),
        P(None, "seq"),
        P("exp"),
        P("seq", None),
        P("exp", None, None, "seq"),
        P("exp", "seq", None),
    )
    out_specs = (P("seq", "exp"), P(None, ("seq", "exp")))
    return jax.shard_map(route, mesh=mesh, in_specs=in_specs, out_specs=out_specs, check_vma=False)
```
